32 devices in a mesh: frame: 4 (over z), space: 8 (over y, x, core).
Axes of the slice: x: 2, y: 2, z: 4, core: 2. Of those that a mesh axis runs over, the one named last changes fastest.
Arguments:
- tokens: bfloat16 [32, 152, 1024], P('space', 'frame'), may hold values from -16 to 16
- tube_count: int32 [8], P('space'), may hold values from 1 to 4, as said below
- ln_gain: float32 [1024], replicated, may hold values from 0.25 to 1.75
- ln_bias: float32 [1024], replicated, may hold values from -3 to 3
- w_qkv: bfloat16 [1024, 1536], replicated, may hold values from -1.5 to 1.5
- w_out: bfloat16 [512, 1024], replicated, may hold values from -0.25 to 0.25
Outputs:
- mixed: bfloat16 [32, 152, 1024], P('space', 'frame')
The draws below stay inside these ranges and needn't reach their ends.
Inputs may be any that keep to these rules, and one draw needn't show every extreme that they name: tube_count[s] is how many of the 4 slots of space index s hold visible tubes; they are the first ones. Some index has all 4, some only 1.
All inputs are finite; a program needn't handle non-finite values.
Results may differ from the reference program's by a relative error of at most 0.005.
Values may be sent and summed in bfloat16 or wider, within the bound.
A program may use at most 128 MiB of HBM per device.

```python
import math
import jax
import jax.numpy as jnp
from jax import lax

D = 1024
HEADS = 8
HD = 64
VIS = 4
TIME = 152
SLOTS = 32
N_SPACE = 8


def draw_tokens(key, part):
    noise_key = jax.random.fold_in(jax.random.fold_in(key, 11), 0)
    drawn = jax.random.normal(noise_key, (SLOTS, TIME, D), jnp.float32)
    return jnp.clip(drawn, -16.0, 16.0).astype(jnp.bfloat16)


def draw_w_qkv(key, part):
    first_key = jax.random.fold_in(jax.random.fold_in(key, 23), 0)
    drawn = jax.random.normal(first_key, (D, 3 * HEADS * HD), jnp.float32) / math.sqrt(D)
    return jnp.clip(drawn, -1.5, 1.5).astype(jnp.bfloat16)


def draw_tube_count(key, part):
    first_key, second_key, third_key, fourth_key = jax.random.split(jax.random.fold_in(key, 37), 4)
    many = jax.random.randint(first_key, (N_SPACE,), 2, VIS + 1)
    chosen = jax.random.randint(second_key, (N_SPACE,), 0, 3) == 0
    counts = jnp.where(chosen, many, 1)
    full_at = jax.random.randint(third_key, (), 0, N_SPACE)
    step_by = jax.random.randint(fourth_key, (), 1, N_SPACE)
    sparse_at = (full_at + step_by) % N_SPACE
    index = jnp.arange(N_SPACE)
    counts = jnp.where(index == full_at, VIS, counts)
    counts = jnp.where(index == sparse_at, 1, counts)
    return counts.astype(jnp.int32)


def bell_draw(stream_key, dims, deviation, bound, held_as=jnp.bfloat16):
    values = deviation * jax.random.normal(stream_key, dims, jnp.float32)
    return jnp.clip(values, min=-bound, max=bound).astype(held_as)


def setup_inputs(seed: int = 0) -> dict:
    splits = jax.random.split(jax.random.key(seed), 7)
    return {
        "tokens": draw_tokens(jax.random.fold_in(splits[6], 71), 0),
        "tube_count": draw_tube_count(jax.random.fold_in(splits[6], 71), 0),
        "ln_gain": jnp.clip(1.0 + 0.15 * jax.random.normal(splits[2], (D,), jnp.float32), 0.25, 1.75),
        "ln_bias": bell_draw(splits[3], (D,), 0.5, 3.0, jnp.float32),
        "w_qkv": draw_w_qkv(jax.random.fold_in(splits[6], 71), 0),
        "w_out": bell_draw(splits[5], (HEADS * HD, D), (HEADS * HD) ** -0.5, 0.25),
    }


EPSILON = 1e-06

def layer_norm(flat, ln_gain, ln_bias):
    values32 = flat.astype(jnp.float32)
    center = values32 - lax.optimization_barrier(jnp.mean(values32, axis=-1, keepdims=True))
    spread = lax.optimization_barrier(jnp.mean(center * center, axis=-1, keepdims=True))
    return (center * lax.rsqrt(spread + EPSILON) * ln_gain + ln_bias).astype(jnp.bfloat16)

def reference(tokens, tube_count, ln_gain, ln_bias, w_qkv, w_out):
    slot_total, time_total, width = tokens.shape
    inner = HEADS * HD
    flat = tokens.reshape(slot_total * time_total, width)
    normed = layer_norm(flat, ln_gain, ln_bias)
    projected = jnp.dot(normed, w_qkv, preferred_element_type=jnp.float32).astype(jnp.bfloat16)
    query_all = projected[:, :inner].astype(jnp.float32).reshape(slot_total, time_total, HEADS, HD)
    key_heads = projected[:, inner:2 * inner].astype(jnp.float32).reshape(-1, HEADS, HD)
    value_heads = projected[:, 2 * inner:].astype(jnp.float32).reshape(-1, HEADS, HD)
    slot_index = jnp.arange(slot_total)
    owner = jnp.arange(N_SPACE)
    slot_count = lax.optimization_barrier(jnp.sum(jnp.where(owner[None, :] == (slot_index // VIS)[:, None], tube_count[None, :], 0), axis=1))
    live_slot = (slot_index % VIS < slot_count).astype(jnp.int32)
    live_int = jnp.broadcast_to(live_slot[:, None], (slot_total, time_total)).reshape(-1)
    live_flat = live_int == 1
    scaling = HD ** (-0.5)

    def one_block(query_block):
        scores = jnp.einsum('qhd,khd->hqk', query_block, key_heads) * scaling
        scores = jnp.where(live_flat[None, None, :], scores, -1e+30)
        highest = lax.optimization_barrier(jnp.max(scores, axis=-1, keepdims=True))
        expw = jnp.exp(scores - highest)
        rounded = lax.optimization_barrier(expw.astype(jnp.bfloat16)).astype(jnp.float32)
        summed = jnp.einsum('hqk,khd->hqd', rounded, value_heads)
        result = summed / lax.optimization_barrier(jnp.sum(expw, axis=-1))[..., None]
        return jnp.transpose(result, (1, 0, 2)).reshape(time_total, inner).astype(jnp.bfloat16)
    attended = lax.map(one_block, query_all).reshape(-1, inner)
    mixed = flat.astype(jnp.float32) + jnp.dot(attended, w_out, preferred_element_type=jnp.float32)
    mixed = jnp.where(live_flat[:, None], mixed, 0.0)
    return mixed.astype(jnp.bfloat16).reshape(slot_total, time_total, width)
```

```python
import functools

import jax
import jax.numpy as jnp
from jax import lax
from jax.experimental import pallas as pl
from jax.experimental.pallas import tpu as pltpu
from jax.sharding import PartitionSpec as P

HEADS = 8
EPSILON = 1e-06
NEG_FILL = -1e30
SUB = 16


def flip(index, bit):
    return index + bit - 2 * bit * lax.rem(lax.div(index, bit), 2)


def bits_of(number):
    return [1 << i for i in range(number.bit_length()) if (number >> i) & 1]


def layer_kernel(
    frames, spaces, slots, times, rows, head_size,
    tok_ref, cnt_ref, gain_ref, bias_ref, wqkv_hbm, wout_hbm, out_ref,
    nrm, wqkv, wout, sbuf, qall, kbuf, vbuf, qexp, vext, acc, best, obuf, abuf,
    w_sem, z_send, z_recv, r_send, r_recv, s_send, s_recv, o_send, o_recv,
):
    f = lax.axis_index("frame")
    s = lax.axis_index("space")
    chips = spaces // 2
    chip_bits = bits_of(chips - 1)
    core_peer = flip(s, 1)
    width_in = kbuf.shape[-1]
    heads = width_in // head_size
    inner = frames * width_in
    live_rows = slots * times

    def frame_at(d):
        return lax.rem(f + d, frames)

    def chip_peer(bit):
        return flip(s, 2 * bit)

    w_copies = [
        pltpu.make_async_copy(wqkv_hbm.at[:, pl.ds(t * inner, inner)], wqkv.at[t], w_sem.at[t])
        for t in range(3)
    ]
    w_copies.append(pltpu.make_async_copy(wout_hbm, wout, w_sem.at[3]))
    for copy in w_copies:
        copy.start()

    barrier = pltpu.get_barrier_semaphore()
    peers = [{"frame": frame_at(d), "space": s} for d in range(1, frames)]
    peers += [{"frame": f, "space": chip_peer(b)} for b in chip_bits]
    peers += [{"frame": f, "space": core_peer}]
    for peer in peers:
        pl.semaphore_signal(barrier, inc=1, device_id=peer, device_id_type=pl.DeviceIdType.MESH)

    count = cnt_ref[0]
    gain = gain_ref[...]
    bias = bias_ref[...]
    first32 = tok_ref[0].astype(jnp.float32)
    for v in range(slots):
        values32 = first32
        if v:
            values32 = jnp.where(v < count, tok_ref[v].astype(jnp.float32), first32)
        center = values32 - jnp.mean(values32, axis=-1, keepdims=True)
        spread = jnp.mean(center * center, axis=-1, keepdims=True)
        normed = center * lax.rsqrt(spread + EPSILON) * gain + bias
        nrm[pl.ds(v * times, times), :] = normed
        if v == 0 and rows > live_rows:
            nrm[pl.ds(live_rows, rows - live_rows), :] = normed[: rows - live_rows]
    normed16 = nrm[...].astype(jnp.bfloat16)

    def z_copy(t, d):
        g = frame_at(d)
        dst = (qall.at[f], kbuf.at[0, 0, f], vbuf.at[0, 0, f])[t]
        return pltpu.make_async_remote_copy(
            src_ref=sbuf.at[t, g], dst_ref=dst,
            send_sem=z_send.at[t, d], recv_sem=z_recv.at[t, frames - d],
            device_id={"frame": g, "space": s}, device_id_type=pl.DeviceIdType.MESH,
        )

    def z_wait(t, d):
        g = frame_at(d)
        dst = (qall.at[g], kbuf.at[0, 0, g], vbuf.at[0, 0, g])[t]
        pltpu.make_async_remote_copy(
            src_ref=sbuf.at[t, g], dst_ref=dst,
            send_sem=z_send.at[t, d], recv_sem=z_recv.at[t, d],
            device_id={"frame": g, "space": s}, device_id_type=pl.DeviceIdType.MESH,
        ).wait_recv()

    bufs = (None, kbuf, vbuf)

    def relay(t, p, bit, d):
        g = frame_at(d)
        return pltpu.make_async_remote_copy(
            src_ref=bufs[t].at[p, 0, g], dst_ref=bufs[t].at[p ^ bit, 0, g],
            send_sem=r_send.at[t - 1, p ^ bit, d], recv_sem=r_recv.at[t - 1, p ^ bit, d],
            device_id={"frame": f, "space": chip_peer(bit)},
            device_id_type=pl.DeviceIdType.MESH,
        )

    def share(t, p, d):
        g = frame_at(d)
        return pltpu.make_async_remote_copy(
            src_ref=bufs[t].at[p, 0, g], dst_ref=bufs[t].at[p, 1, g],
            send_sem=s_send.at[t - 1, p, d], recv_sem=s_recv.at[t - 1, p, d],
            device_id={"frame": f, "space": core_peer},
            device_id_type=pl.DeviceIdType.MESH,
        )

    def path_bit(t, p):
        return bits_of(p)[0] if t == 1 else bits_of(p)[-1]

    def onward(t, p, d):
        copies = []
        for bit in chip_bits:
            if not p & bit and path_bit(t, p ^ bit) == bit:
                copies.append(relay(t, p, bit, d))
        copies.append(share(t, p, d))
        return copies

    in_flight = []

    def launch(copies):
        for copy in copies:
            copy.start()
            in_flight.append(copy)

    scaling = head_size ** (-0.5)
    row_ids = lax.broadcasted_iota(jnp.int32, (rows, 1), 0)
    count32 = count.astype(jnp.float32)
    for t in range(3):
        w_copies[t].wait()
        product = jnp.dot(normed16, wqkv[t], preferred_element_type=jnp.float32)
        if t == 0:
            product = product.astype(jnp.bfloat16).astype(jnp.float32) * scaling
        if t == 2:
            product = jnp.where(row_ids < live_rows, product, count32)
        product = product.astype(jnp.bfloat16)
        for g in range(frames):
            sbuf[t, g] = product[:, g * width_in:(g + 1) * width_in]
        if t == 0:
            qall[f] = sbuf[t, f]
        else:
            bufs[t][0, 0, f] = sbuf[t, f]
        if t == 0:
            pl.semaphore_wait(barrier, len(peers))
        launch([z_copy(t, d) for d in range(1, frames)])
        if t:
            launch(onward(t, 0, 0))

    for d in range(1, frames):
        z_wait(0, d)
    lane_head = lax.broadcasted_iota(jnp.int32, (1, width_in), 1)
    for h in range(heads):
        mine = (lane_head >= h * head_size) & (lane_head < (h + 1) * head_size)
        for g in range(frames):
            block = qall[g].astype(jnp.float32)
            qexp[pl.ds((h * frames + g) * rows, rows), :] = jnp.where(mine, block, 0.0).astype(
                jnp.bfloat16
            )

    for t in (1, 2):
        for d in range(1, frames):
            z_wait(t, d)
            launch(onward(t, 0, d))

    total_rows = heads * frames * rows
    keys = frames * rows
    step_rows = 2 * rows
    steps = total_rows // step_rows
    key_ids = lax.broadcasted_iota(jnp.int32, (rows, width_in), 0).astype(jnp.float32)

    def fold(p, j, first):
        for g in range(frames):
            values = vbuf[p, j, g].astype(jnp.float32)
            limit = values[rows - 8:rows][0:1] * float(times)
            live = key_ids < limit
            vext[pl.ds(g * rows, rows), 0:width_in] = jnp.where(live, values, 0.0).astype(
                jnp.bfloat16
            )
            vext[pl.ds(g * rows, rows), width_in:2 * width_in] = jnp.where(
                live, 1.0, 0.0
            ).astype(jnp.bfloat16)

        def step(i, carry):
            part = pl.ds(pl.multiple_of(i * step_rows, SUB), step_rows)
            scores = lax.dot_general(
                qexp[part, :], kbuf[p, j].reshape(keys, width_in),
                (((1,), (1,)), ((), ())), preferred_element_type=jnp.float32,
            )
            top = jnp.max(scores, axis=-1, keepdims=True)
            if not first:
                old = best[part, :][:, 0:1]
                top = jnp.maximum(top, old)
            weights = jnp.exp(scores - top).astype(jnp.bfloat16)
            added = jnp.dot(weights, vext[...], preferred_element_type=jnp.float32)
            if first:
                acc[part, :] = added
            else:
                acc[part, :] = acc[part, :] * jnp.exp(old - top) + added
            best[part, :] = jnp.broadcast_to(top, (step_rows, best.shape[1]))
            return carry

        lax.fori_loop(0, steps, step, 0, unroll=2 if steps % 2 == 0 else 1)

    fold(0, 0, True)

    def arrive(p):
        for t in (1, 2):
            for d in range(frames):
                relay(t, p ^ path_bit(t, p), path_bit(t, p), d).wait_recv()
                launch(onward(t, p, d))

    def arrive_shared(p):
        for t in (1, 2):
            for d in range(frames):
                share(t, p, d).wait_recv()

    order = sorted(range(1, chips), key=lambda p: (len(bits_of(p)), p))
    waves = {}
    for p in order:
        waves.setdefault(len(bits_of(p)), []).append(p)
    pending = [0]
    for level in sorted(waves):
        for p in waves[level]:
            arrive(p)
        for p in pending:
            arrive_shared(p)
            fold(p, 1, False)
        for p in waves[level]:
            fold(p, 0, False)
        pending = waves[level]
    for p in pending:
        arrive_shared(p)
        fold(p, 1, False)

    def o_copy(d, dst_frame):
        g = frame_at(d)
        return pltpu.make_async_remote_copy(
            src_ref=obuf.at[g], dst_ref=abuf.at[dst_frame],
            send_sem=o_send.at[d], recv_sem=o_recv.at[frames - d],
            device_id={"frame": g, "space": s}, device_id_type=pl.DeviceIdType.MESH,
        )

    for g in range(frames):
        joined = None
        for h in range(heads):
            part = pl.ds((h * frames + g) * rows, rows)
            value = acc[part, 0:width_in] / acc[part, width_in:2 * width_in]
            if joined is None:
                joined = value
            else:
                joined = jnp.where(lane_head < h * head_size, joined, value)
        obuf[g] = joined.astype(jnp.bfloat16)
    abuf[f] = obuf[f]
    launch([o_copy(d, f) for d in range(1, frames)])
    w_copies[3].wait()
    for d in range(1, frames):
        g = frame_at(d)
        pltpu.make_async_remote_copy(
            src_ref=obuf.at[g], dst_ref=abuf.at[g],
            send_sem=o_send.at[d], recv_sem=o_recv.at[d],
            device_id={"frame": g, "space": s}, device_id_type=pl.DeviceIdType.MESH,
        ).wait_recv()
    attended = jnp.concatenate([abuf[g] for g in range(frames)], axis=1)
    nrm[...] = jnp.dot(attended, wout[...], preferred_element_type=jnp.float32)
    for v in range(slots):
        mixed = tok_ref[v].astype(jnp.float32) + nrm[pl.ds(v * times, times), :]
        out_ref[v] = jnp.where(v < count, mixed, 0.0).astype(jnp.bfloat16)
    for copy in in_flight:
        copy.wait_send()


def on_device(frames, spaces, tokens, tube_count, ln_gain, ln_bias, w_qkv, w_out):
    slots, times, width = tokens.shape
    inner = w_out.shape[0]
    head_size = inner // HEADS
    width_in = inner // frames
    rows = -(-(slots * times + 1) // SUB) * SUB
    chips = spaces // 2
    heads = width_in // head_size
    total_rows = heads * frames * rows
    bf16, f32 = jnp.bfloat16, jnp.float32
    vmem = pl.BlockSpec(memory_space=pltpu.VMEM)
    hbm = pl.BlockSpec(memory_space=pl.ANY)
    dma = pltpu.SemaphoreType.DMA
    return pl.pallas_call(
        functools.partial(layer_kernel, frames, spaces, slots, times, rows, head_size),
        out_shape=jax.ShapeDtypeStruct(tokens.shape, bf16),
        in_specs=[vmem, pl.BlockSpec(memory_space=pltpu.SMEM), vmem, vmem, hbm, hbm],
        out_specs=vmem,
        scratch_shapes=[
            pltpu.VMEM((rows, width), f32),
            pltpu.VMEM((3, width, inner), bf16),
            pltpu.VMEM((inner, width), bf16),
            pltpu.VMEM((3, frames, rows, width_in), bf16),
            pltpu.VMEM((frames, rows, width_in), bf16),
            pltpu.VMEM((chips, 2, frames, rows, width_in), bf16),
            pltpu.VMEM((chips, 2, frames, rows, width_in), bf16),
            pltpu.VMEM((total_rows, width_in), bf16),
            pltpu.VMEM((frames * rows, 2 * width_in), bf16),
            pltpu.VMEM((total_rows, 2 * width_in), f32),
            pltpu.VMEM((total_rows, 128), f32),
            pltpu.VMEM((frames, rows, width_in), bf16),
            pltpu.VMEM((frames, rows, width_in), bf16),
            dma((4,)),
            dma((3, frames)), dma((3, frames)),
            dma((2, chips, frames)), dma((2, chips, frames)),
            dma((2, chips, frames)), dma((2, chips, frames)),
            dma((frames,)), dma((frames,)),
        ],
        compiler_params=pltpu.CompilerParams(
            collective_id=0, has_side_effects=True, vmem_limit_bytes=56 * 1024 * 1024
        ),
    )(tokens, tube_count, ln_gain.reshape(1, width), ln_bias.reshape(1, width), w_qkv, w_out)


def solution(mesh):
    in_specs = (P("space", "frame", None), P("space"), P(), P(), P(), P())
    out_specs = P("space", "frame", None)
    body = functools.partial(on_device, mesh.shape["frame"], mesh.shape["space"])
    return jax.shard_map(
        body, mesh=mesh, in_specs=in_specs, out_specs=out_specs, check_vma=False
    )
```

```python
import functools

import jax
import jax.numpy as jnp
from jax import lax
from jax.experimental import pallas as pl
from jax.experimental.pallas import tpu as pltpu
from jax.sharding import PartitionSpec as P

HEADS = 8
EPSILON = 1e-06
SUB = 16


def flip(index, bit):
    return index + bit - 2 * bit * lax.rem(lax.div(index, bit), 2)


def bits_of(number):
    return [1 << i for i in range(number.bit_length()) if (number >> i) & 1]


def layer_kernel(
    frames, spaces, slots, times, rows, head_size,
    tok_ref, cnt_ref, gain_ref, bias_ref, wqkv_hbm, wout_hbm, out_ref,
    nrm, wqkv, wout, qsend, kvsend, qall, kvbuf, qexp, vext, acc, best, obuf, abuf,
    w_sem, z_send, z_recv, r_send, r_recv, s_send, s_recv, o_send, o_recv,
):
    f = lax.axis_index("frame")
    s = lax.axis_index("space")
    chips = spaces // 2
    chip_bits = bits_of(chips - 1)
    core_peer = flip(s, 1)
    width_in = kvbuf.shape[-1]
    heads = width_in // head_size
    inner = frames * width_in
    live_rows = slots * times

    def frame_at(d):
        return lax.rem(f + d, frames)

    def chip_peer(bit):
        return flip(s, 2 * bit)

    w_copies = [
        pltpu.make_async_copy(wqkv_hbm.at[:, pl.ds(t * inner, inner)], wqkv.at[t], w_sem.at[t])
        for t in range(3)
    ]
    w_copies.append(pltpu.make_async_copy(wout_hbm, wout, w_sem.at[3]))
    for t in (1, 2, 0, 3):
        w_copies[t].start()

    barrier = pltpu.get_barrier_semaphore()
    peers = [{"frame": frame_at(d), "space": s} for d in range(1, frames)]
    peers += [{"frame": f, "space": chip_peer(b)} for b in chip_bits]
    peers += [{"frame": f, "space": core_peer}]
    for peer in peers:
        pl.semaphore_signal(barrier, inc=1, device_id=peer, device_id_type=pl.DeviceIdType.MESH)

    count = cnt_ref[0]
    gain = gain_ref[...]
    bias = bias_ref[...]
    slot_live = lax.broadcasted_iota(jnp.int32, (slots, 1), 0) < count
    for i in range(times):
        token32 = tok_ref[i].astype(jnp.float32)
        nrm[pl.ds(i * slots, slots), :] = jnp.where(slot_live, token32, token32[0:1])
    spare = rows - live_rows
    nrm[pl.ds(live_rows, spare), :] = nrm[pl.ds(0, spare), :]
    values32 = nrm[...]
    center = values32 - jnp.mean(values32, axis=-1, keepdims=True)
    spread = jnp.mean(center * center, axis=-1, keepdims=True)
    normed16 = (center * lax.rsqrt(spread + EPSILON) * gain + bias).astype(jnp.bfloat16)

    def remote(src, dst, send_sem, recv_sem, peer):
        return pltpu.make_async_remote_copy(
            src_ref=src, dst_ref=dst, send_sem=send_sem, recv_sem=recv_sem,
            device_id=peer, device_id_type=pl.DeviceIdType.MESH,
        )

    def z_copy(kv, d, home):
        g = frame_at(d)
        src = kvsend.at[g] if kv else qsend.at[g]
        dst = kvbuf.at[home, :, 0, 0] if kv else qall.at[home]
        return src, dst, {"frame": g, "space": s}

    def z_start(kv, d):
        src, dst, peer = z_copy(kv, d, f)
        return remote(src, dst, z_send.at[kv, d], z_recv.at[kv, frames - d], peer)

    def z_wait(kv, d):
        src, dst, peer = z_copy(kv, d, frame_at(d))
        remote(src, dst, z_send.at[kv, d], z_recv.at[kv, d], peer).wait_recv()

    def routes(p):
        low, high = bits_of(p)[0], bits_of(p)[-1]
        return [(2, low)] if low == high else [(0, low), (1, high)]

    def part_of(g, part, p, j):
        return kvbuf.at[g, :, p, j] if part == 2 else kvbuf.at[g, part, p, j]

    def relay(part, p, bit, d):
        g = frame_at(d)
        slot = part % 2
        return remote(
            part_of(g, part, p, 0), part_of(g, part, p ^ bit, 0),
            r_send.at[slot, p ^ bit, d], r_recv.at[slot, p ^ bit, d],
            {"frame": f, "space": chip_peer(bit)},
        )

    def share(p, d):
        g = frame_at(d)
        return remote(
            part_of(g, 2, p, 0), part_of(g, 2, p, 1), s_send.at[p, d], s_recv.at[p, d],
            {"frame": f, "space": core_peer},
        )

    def onward(p, d):
        copies = []
        for bit in chip_bits:
            if not p & bit:
                copies += [relay(part, p, bit, d) for part, by in routes(p ^ bit) if by == bit]
        return copies + [share(p, d)]

    in_flight = []

    def launch(copies):
        for copy in copies:
            copy.start()
            in_flight.append(copy)

    far = sorted(range(1, frames), key=lambda d: (min(d, frames - d), d))
    scaling = head_size ** (-0.5)
    row_ids = lax.broadcasted_iota(jnp.int32, (rows, 1), 0)
    count32 = count.astype(jnp.float32)
    for t in (1, 2, 0):
        w_copies[t].wait()
        product = jnp.dot(normed16, wqkv[t], preferred_element_type=jnp.float32)
        if t == 0:
            product = product.astype(jnp.bfloat16).astype(jnp.float32) * scaling
        if t == 2:
            product = jnp.where(row_ids < live_rows, product, count32)
        product = product.astype(jnp.bfloat16)
        for g in range(frames):
            piece = product[:, g * width_in:(g + 1) * width_in]
            if t == 0:
                qsend[g] = piece
            else:
                kvsend[g, t - 1] = piece
        if t == 0:
            qall[f] = qsend[f]
        else:
            kvbuf[f, t - 1, 0, 0] = kvsend[f, t - 1]
        if t == 2:
            pl.semaphore_wait(barrier, len(peers))
            launch([z_start(1, d) for d in far])
            launch(onward(0, 0))
    launch([z_start(0, d) for d in far])

    lane_head = lax.broadcasted_iota(jnp.int32, (1, width_in), 1)
    keys = spaces * rows
    frame_rows = heads * rows
    row_key = lax.broadcasted_iota(jnp.int32, (rows, width_in), 0)
    slot_key = jnp.where(row_key < live_rows, lax.rem(row_key, slots), slots).astype(jnp.float32)

    def prepare(d):
        g = frame_at(d)
        for p in range(chips):
            for j in range(2):
                values = kvbuf[g, 1, p, j].astype(jnp.float32)
                live = slot_key < values[rows - 8:rows][0:1]
                part = pl.ds((2 * p + j) * rows, rows)
                vext[part, 0:width_in] = jnp.where(live, values, 0.0).astype(jnp.bfloat16)
                vext[part, width_in:2 * width_in] = jnp.where(live, 1.0, 0.0).astype(jnp.bfloat16)

    def fold(d, first, start, count):
        size = count * frame_rows
        part = pl.ds(pl.multiple_of(start * frame_rows, SUB), size)
        scores = lax.dot_general(
            qexp[part, :], kvbuf[frame_at(d), 0].reshape(keys, width_in),
            (((1,), (1,)), ((), ())), preferred_element_type=jnp.float32,
        )
        top = jnp.max(scores, axis=-1, keepdims=True)
        if not first:
            old = best[part, :][:, 0:1]
            top = jnp.maximum(top, old)
        weights = jnp.exp(scores - top).astype(jnp.bfloat16)
        added = jnp.dot(weights, vext[...], preferred_element_type=jnp.float32)
        if first:
            acc[part, :] = added
        else:
            acc[part, :] = acc[part, :] * jnp.exp(old - top) + added
        best[part, :] = jnp.broadcast_to(top, (size, best.shape[1]))

    order = sorted(range(1, chips), key=lambda p: (len(bits_of(p)), p))

    sequence = [0] + far
    levels = len(chip_bits)
    done = set()

    def once(what, n, level=0):
        if n >= len(sequence) or (what, n, level) in done:
            return
        done.add((what, n, level))
        d = sequence[n]
        if what == "frame" and n:
            z_wait(1, d)
            launch(onward(0, d))
        if what == "chip":
            for p in order:
                if len(bits_of(p)) == level:
                    for part, bit in routes(p):
                        relay(part, p ^ bit, bit, d).wait_recv()
                    launch(onward(p, d))
        if what == "core":
            for p in range(chips):
                share(p, d).wait_recv()

    def chip_levels(n, low, high):
        for level in range(low, high + 1):
            once("chip", n, level)

    def o_copy(d, home, arrival):
        g = frame_at(d)
        return remote(
            obuf.at[g], abuf.at[home], o_send.at[d], o_recv.at[arrival], {"frame": g, "space": s}
        )

    def finish(d):
        g = frame_at(d)
        joined = None
        for h in range(heads):
            part = pl.ds(pl.multiple_of(g * frame_rows + h * rows, SUB), rows)
            value = acc[part, 0:width_in] / acc[part, width_in:2 * width_in]
            joined = value if h == 0 else jnp.where(lane_head < h * head_size, joined, value)
        obuf[g] = joined.astype(jnp.bfloat16)
        if d:
            launch([o_copy(d, f, frames - d)])
        else:
            abuf[f] = obuf[f]

    once("frame", 1)
    once("chip", 0, 1)
    once("frame", 2)
    once("chip", 1, 1)
    chip_levels(0, 2, levels)
    for n in range(3, frames):
        once("frame", n)
    chip_levels(1, 2, levels)
    once("chip", 2, 1)
    for d in far:
        z_wait(0, d)
    for h in range(heads):
        mine = (lane_head >= h * head_size) & (lane_head < (h + 1) * head_size)
        for g in range(frames):
            block = qall[g].astype(jnp.float32)
            qexp[pl.ds((g * heads + h) * rows, rows), :] = jnp.where(mine, block, 0.0).astype(
                jnp.bfloat16
            )

    once("core", 0)
    for n in range(frames - 1):
        prepare(sequence[n])
        half = frames // 2
        fold(sequence[n], n == 0, 0, half)
        once("chip", n + 1, 1)
        if n:
            once("chip", n + 2, 1)
            chip_levels(n + 1, 2, levels)
        fold(sequence[n], n == 0, half, frames - half)
        once("frame", n + 3)
        chip_levels(n + 1, 1, levels)
        once("chip", n + 2, 1)
        once("core", n + 1)
    prepare(sequence[-1])
    for d in far[::-1] + [0]:
        fold(sequence[-1], frames == 1, frame_at(d), 1)
        finish(d)

    w_copies[3].wait()
    for d in far:
        o_copy(d, frame_at(d), d).wait_recv()
    attended = jnp.concatenate([abuf[g] for g in range(frames)], axis=1)
    nrm[...] = jnp.dot(attended, wout[...], preferred_element_type=jnp.float32)
    for i in range(times):
        mixed = tok_ref[i].astype(jnp.float32) + nrm[pl.ds(i * slots, slots), :]
        out_ref[i] = jnp.where(slot_live, mixed, 0.0).astype(jnp.bfloat16)
    for copy in in_flight:
        copy.wait_send()


def on_device(frames, spaces, tokens, tube_count, ln_gain, ln_bias, w_qkv, w_out):
    slots, times, width = tokens.shape
    inner = w_out.shape[0]
    head_size = inner // HEADS
    width_in = inner // frames
    rows = -(-(slots * times + 1) // SUB) * SUB
    chips = spaces // 2
    heads = width_in // head_size
    total_rows = heads * frames * rows
    bf16, f32 = jnp.bfloat16, jnp.float32
    vmem = pl.BlockSpec(memory_space=pltpu.VMEM)
    hbm = pl.BlockSpec(memory_space=pl.ANY)
    dma = pltpu.SemaphoreType.DMA
    mixed = pl.pallas_call(
        functools.partial(layer_kernel, frames, spaces, slots, times, rows, head_size),
        out_shape=jax.ShapeDtypeStruct((times, slots, width), bf16),
        in_specs=[vmem, pl.BlockSpec(memory_space=pltpu.SMEM), vmem, vmem, hbm, hbm],
        out_specs=vmem,
        scratch_shapes=[
            pltpu.VMEM((rows, width), f32),
            pltpu.VMEM((3, width, inner), bf16),
            pltpu.VMEM((inner, width), bf16),
            pltpu.VMEM((frames, rows, width_in), bf16),
            pltpu.VMEM((frames, 2, rows, width_in), bf16),
            pltpu.VMEM((frames, rows, width_in), bf16),
            pltpu.VMEM((frames, 2, chips, 2, rows, width_in), bf16),
            pltpu.VMEM((total_rows, width_in), bf16),
            pltpu.VMEM((spaces * rows, 2 * width_in), bf16),
            pltpu.VMEM((total_rows, 2 * width_in), f32),
            pltpu.VMEM((total_rows, 128), f32),
            pltpu.VMEM((frames, rows, width_in), bf16),
            pltpu.VMEM((frames, rows, width_in), bf16),
            dma((4,)),
            dma((2, frames)), dma((2, frames)),
            dma((2, chips, frames)), dma((2, chips, frames)),
            dma((chips, frames)), dma((chips, frames)),
            dma((frames,)), dma((frames,)),
        ],
        compiler_params=pltpu.CompilerParams(
            collective_id=0, has_side_effects=True, vmem_limit_bytes=56 * 1024 * 1024
        ),
    )(
        jnp.transpose(tokens, (1, 0, 2)), tube_count,
        ln_gain.reshape(1, width), ln_bias.reshape(1, width), w_qkv, w_out,
    )
    return jnp.transpose(mixed, (1, 0, 2))


def solution(mesh):
    in_specs = (P("space", "frame", None), P("space"), P(), P(), P(), P())
    out_specs = P("space", "frame", None)
    body = functools.partial(on_device, mesh.shape["frame"], mesh.shape["space"])
    return jax.shard_map(
        body, mesh=mesh, in_specs=in_specs, out_specs=out_specs, check_vma=False
    )
```
